32 devices in a mesh: seq: 8 (over z, x), head: 4 (over y, core).
Axes of the slice: x: 2, y: 2, z: 4, core: 2. Of those that a mesh axis runs over, the one named last changes fastest.
Arguments:
- q_latent: bfloat16 [2048, 1536], P('seq', 'head'), may hold values from -6 to 6
- kv_latent: bfloat16 [2048, 512], P('seq', 'head'), may hold values from -6 to 6
- k_rope: bfloat16 [2048, 64], P('seq'), may hold values from -6 to 6
- segment_ids: int32 [2048], P('seq'), may hold values from 0 to 7, as said below
- w_q_nope: bfloat16 [1536, 16384], P('seq', 'head'), may hold values from -6 to 6
- w_q_rope: bfloat16 [1536, 8192], P('seq', 'head'), may hold values from -6 to 6
- w_kv_nope: bfloat16 [512, 16384], P('seq', 'head'), may hold values from -6 to 6
- threshold: float32 [1], replicated, may hold values from 3.5 to 5.5
Outputs:
- new_q_nope: bfloat16 [1536, 16384], P('seq', 'head')
- new_q_rope: bfloat16 [1536, 8192], P('seq', 'head')
- new_kv_nope: bfloat16 [512, 16384], P('seq', 'head')
- head_max: float32 [128], P('head')
- row_max: float32 [2048, 128], P('seq', 'head')
The draws below stay inside these ranges and needn't reach their ends.
Inputs may be any that keep to these rules, and one draw needn't show every extreme that they name: segment_ids never fall along the tokens and each document has 1 to 768 tokens.
All inputs are finite; a program needn't handle non-finite values.
Results may differ from the reference program's by a relative error of at most 0.0034.
Values may be sent and summed in bfloat16 or wider, within the bound.
A program may use at most 128 MiB of HBM per device.

```python
import math
import jax
import jax.numpy as jnp
from jax import lax

H = 128
D_NOPE = 128
D_ROPE = 64
QLORA = 1536
KVLORA = 512
TOK_DEV = 256
REACH = 3
TOKENS = 2048
N_SEQ = 8


def draw_segment_ids(key, part):
    count_blocks = TOKENS // TOK_DEV
    offsets = jax.random.randint(jax.random.fold_in(key, 11), (count_blocks,), 1, TOK_DEV - 1)
    position = jnp.arange(TOKENS, dtype=jnp.int32)
    block = position // TOK_DEV
    within = position % TOK_DEV
    regular = (within == offsets[block]) & (block <= count_blocks - 4)
    long_start = (count_blocks - 3) * TOK_DEV - 1
    flags = regular | (position == 0) | (position == long_start) | (position == TOKENS - 1)
    return (jnp.cumsum(flags.astype(jnp.int32)) - 1).astype(jnp.int32)


def block_scale(stream_key, shape, pieces, low, top_value):
    level, own = 1.0, jax.random.fold_in(stream_key, 6)
    for dim, parts in pieces:
        heights = jnp.exp(jax.random.uniform(jax.random.fold_in(own, dim), (parts,), jnp.float32, low / len(pieces), top_value / len(pieces)))
        level = level * jnp.repeat(heights, shape[dim] // parts).reshape([-1 if axis == dim else 1 for axis in range(len(shape))])
    return level


def gaussian(own_key, shape, scale, bound, split=(), kind=jnp.bfloat16):
    entries = jax.random.normal(own_key, shape, jnp.float32) * scale
    if len(split) > 0:
        entries = block_scale(own_key, shape, split, -0.22, 0.18) * entries
    return jnp.clip(entries, min=-bound, max=bound).astype(kind)


def setup_inputs(seed: int = 0) -> dict:
    key_list = jax.random.split(jax.random.key(seed), 9)
    q_latent = gaussian(key_list[0], (TOKENS, QLORA), 1.0, 6.0, ((0, 8), (1, 4)))
    kv_latent = gaussian(key_list[1], (TOKENS, KVLORA), 1.0, 6.0, ((0, 8), (1, 4)))
    k_rope = gaussian(key_list[2], (TOKENS, D_ROPE), 1.0, 6.0, ((0, 8),))
    segment_ids = draw_segment_ids(jax.random.fold_in(key_list[8], 71), 0)
    w_q_nope = gaussian(key_list[4], (QLORA, H * D_NOPE), 1.0, 6.0, ((0, 8), (1, 4)))
    w_q_rope = gaussian(key_list[5], (QLORA, H * D_ROPE), 1.0, 6.0, ((0, 8), (1, 4)))
    w_kv_nope = gaussian(key_list[6], (KVLORA, H * D_NOPE), 1.0, 6.0, ((0, 8), (1, 4)))
    threshold = jnp.clip(jax.random.uniform(key_list[7], (1,), jnp.float32, 3.5, 5.5), 3.5, 5.5)
    return dict(q_latent=q_latent, kv_latent=kv_latent, k_rope=k_rope, segment_ids=segment_ids, w_q_nope=w_q_nope, w_q_rope=w_q_rope, w_kv_nope=w_kv_nope, threshold=threshold)


def reference(q_latent, kv_latent, k_rope, segment_ids, w_q_nope, w_q_rope, w_kv_nope, threshold):
    q_scale = 1.0 / math.sqrt(QLORA)
    k_scale = 1.0 / math.sqrt(KVLORA)
    score_scale = 1.0 / math.sqrt(D_NOPE + D_ROPE)
    window = (REACH + 1) * TOK_DEV

    def advance(carry, block):
        old_nope, old_rope, old_seg = carry
        start = (block * TOK_DEV).astype(jnp.int32)
        q_lat = lax.dynamic_slice_in_dim(q_latent, start, TOK_DEV, 0)
        kv_lat = lax.dynamic_slice_in_dim(kv_latent, start, TOK_DEV, 0)
        rope_own = lax.dynamic_slice_in_dim(k_rope, start, TOK_DEV, 0)
        seg_own = lax.dynamic_slice_in_dim(segment_ids, start, TOK_DEV, 0)
        query_nope = (jnp.dot(q_lat, w_q_nope, preferred_element_type=jnp.float32) * q_scale).astype(jnp.bfloat16).reshape(TOK_DEV, H, D_NOPE)
        query_rope = (jnp.dot(q_lat, w_q_rope, preferred_element_type=jnp.float32) * q_scale).astype(jnp.bfloat16).reshape(TOK_DEV, H, D_ROPE)
        key_own = (jnp.dot(kv_lat, w_kv_nope, preferred_element_type=jnp.float32) * k_scale).astype(jnp.bfloat16)
        all_nope = jnp.concatenate([old_nope, key_own[None]], 0)
        all_rope = jnp.concatenate([old_rope, rope_own[None]], 0)
        all_seg = jnp.concatenate([old_seg, seg_own[None]], 0)
        keys_nope = all_nope.reshape(window, H, D_NOPE)
        keys_rope = all_rope.reshape(window, D_ROPE)
        keys_seg = all_seg.reshape(window)
        query_pos = start + jnp.arange(TOK_DEV, dtype=jnp.int32)
        key_pos = start - REACH * TOK_DEV + jnp.arange(window, dtype=jnp.int32)
        allowed = (seg_own[:, None] == keys_seg[None, :]) & (key_pos[None, :] <= query_pos[:, None]) & (key_pos[None, :] >= 0)
        nope = jnp.einsum('qhd,khd->hqk', query_nope.astype(jnp.float32), keys_nope.astype(jnp.float32))
        rope = jnp.einsum('qhd,kd->hqk', query_rope.astype(jnp.float32), keys_rope.astype(jnp.float32))
        scores = (nope + rope) * score_scale
        block_rows = lax.optimization_barrier(jnp.max(jnp.where(allowed[None], scores, jnp.float32(-1e+30)), axis=2))
        return ((all_nope[1:], all_rope[1:], all_seg[1:]), block_rows.T)
    init = (jnp.zeros((REACH, TOK_DEV, H * D_NOPE), jnp.bfloat16), jnp.zeros((REACH, TOK_DEV, D_ROPE), jnp.bfloat16), jnp.zeros((REACH, TOK_DEV), jnp.int32))
    carry, rows = lax.scan(advance, init, jnp.arange(N_SEQ, dtype=jnp.int32))
    row_max = rows.reshape(TOKENS, H)
    head_max = lax.optimization_barrier(jnp.max(row_max, axis=0))
    clip = threshold[0] / jnp.maximum(head_max, threshold[0])
    root = jnp.sqrt(clip)
    new_q_nope = (w_q_nope.astype(jnp.float32) * jnp.repeat(root, D_NOPE)[None, :]).astype(jnp.bfloat16)
    new_q_rope = (w_q_rope.astype(jnp.float32) * jnp.repeat(clip, D_ROPE)[None, :]).astype(jnp.bfloat16)
    new_kv_nope = (w_kv_nope.astype(jnp.float32) * jnp.repeat(root, D_NOPE)[None, :]).astype(jnp.bfloat16)
    return (new_q_nope, new_q_rope, new_kv_nope, head_max, row_max)
```

```python
import functools
import math

import jax
import jax.numpy as jnp
from jax import lax
from jax.experimental import pallas as pl
from jax.experimental.pallas import tpu as pltpu
from jax.sharding import PartitionSpec as P

D_NOPE = 128
D_ROPE = 64
QLORA = 1536
KVLORA = 512
REACH = 3


def as_sent(value):
    return jax.tree.map(lambda a: a.astype(jnp.bfloat16) if a.dtype == jnp.float32 else a, value)


def from_partner(value, axis, stride):
    mask = 2**stride
    pairs = [(source, source ^ mask) for source in range(lax.axis_size(axis))]
    return lax.ppermute(value, axis, pairs)


def shifted(block, axis, distance):
    devices = range(lax.axis_size(axis))
    route = [(i - distance, i) for i in devices if i - distance in devices]
    return lax.ppermute(block, axis, route)


def score_max(query_nope, query_rope, key_nope, key_rope, allowed):
    nope = jnp.einsum("qhd,khd->hqk", query_nope, key_nope, preferred_element_type=jnp.float32)
    rope = jnp.einsum("qhd,kd->hqk", query_rope, key_rope, preferred_element_type=jnp.float32)
    scores = (nope + rope) * (1.0 / math.sqrt(D_NOPE + D_ROPE))
    return jnp.max(jnp.where(allowed[None], scores, jnp.float32(-1e30)), axis=2)


def masked_max(compute, operands):
    return compute(*operands)


def spread_columns(weight, width, quarter, copies):
    pieces = weight.reshape(weight.shape[0], 4, quarter * width).transpose(1, 0, 2)
    return jnp.tile(pieces, (copies, 1, 1))


def grouped_body(q_latent, kv_latent, k_rope, segment_ids, w_q_nope, w_q_rope, w_kv_nope, threshold):
    q_whole, kv_whole = (
        lax.all_gather(q_latent, "head", axis=1, tiled=True),
        lax.all_gather(kv_latent, "head", axis=1, tiled=True),
    )
    rows = q_whole.shape[0]
    heads = w_q_nope.shape[1] // D_NOPE
    q_scale = 1.0 / math.sqrt(QLORA)
    k_scale = 1.0 / math.sqrt(KVLORA)
    place = lax.axis_index("seq")
    quarter = heads // 4
    copies = lax.axis_size("seq") // 4
    slot = place % 4
    sent = (
        spread_columns(w_q_nope, D_NOPE, quarter, copies),
        spread_columns(w_q_rope, D_ROPE, quarter, copies),
        spread_columns(w_kv_nope, D_NOPE, quarter, copies),
    )
    got_nope, got_rope, got_kv = (
        lax.all_to_all(sent[0], "seq", split_axis=0, concat_axis=1, tiled=True),
        lax.all_to_all(sent[1], "seq", split_axis=0, concat_axis=1, tiled=True),
        lax.all_to_all(sent[2], "seq", split_axis=0, concat_axis=1, tiled=True),
    )
    sub_nope = got_nope.reshape(QLORA, quarter * D_NOPE)
    sub_rope = got_rope.reshape(QLORA, quarter * D_ROPE)
    sub_kv = got_kv.reshape(KVLORA, quarter * D_NOPE)
    group = (q_whole, kv_whole, k_rope)
    for level in range(2):
        partner = jax.tree.map(
            lambda part, own: part.astype(own.dtype),
            from_partner(as_sent(group), "seq", level),
            group,
        )
        upper = place // (1 << level) % 2 == 1
        group = tuple(
            (
                jnp.where(
                    upper, jnp.concatenate([other, mine], 0), jnp.concatenate([mine, other], 0)
                )
                for mine, other in zip(group, partner)
            )
        )
    group_q, group_kv, group_rope = group
    early_kv, early_rope = shifted(
        (group_kv[(4 - REACH) * rows :], group_rope[(4 - REACH) * rows :]), "seq", 4
    )
    keys_kv = jnp.concatenate([early_kv, group_kv], 0)
    keys_rope = jnp.concatenate([early_rope, group_rope], 0)
    key_nope = (
        (jnp.dot(keys_kv, sub_kv, preferred_element_type=jnp.float32) * k_scale)
        .astype(jnp.bfloat16)
        .reshape(keys_kv.shape[0], quarter, D_NOPE)
    )
    query_nope = (
        (jnp.dot(group_q, sub_nope, preferred_element_type=jnp.float32) * q_scale)
        .astype(jnp.bfloat16)
        .reshape(4 * rows, quarter, D_NOPE)
    )
    query_rope = (
        (jnp.dot(group_q, sub_rope, preferred_element_type=jnp.float32) * q_scale)
        .astype(jnp.bfloat16)
        .reshape(4 * rows, quarter, D_ROPE)
    )
    all_segs = lax.all_gather(segment_ids, "seq", axis=0, tiled=True)
    padded_segs = jnp.concatenate([jnp.full((REACH * rows,), -1, jnp.int32), all_segs], 0)
    first = place // 4 * 4
    window = (REACH + 1) * rows
    block_rows = []
    for local in range(4):
        block = first + local
        query_seg = lax.dynamic_slice_in_dim(all_segs, block * rows, rows, 0)
        key_seg = lax.dynamic_slice_in_dim(padded_segs, block * rows, window, 0)
        query_pos = block * rows + jnp.arange(rows, dtype=jnp.int32)
        key_pos = (block - REACH) * rows + jnp.arange(window, dtype=jnp.int32)
        allowed = (
            (query_seg[:, None] == key_seg[None, :])
            & (key_pos[None, :] <= query_pos[:, None])
            & (key_pos[None, :] >= 0)
        )
        operands = (
            query_nope[local * rows : (local + 1) * rows],
            query_rope[local * rows : (local + 1) * rows],
            key_nope[local * rows : local * rows + window],
            keys_rope[local * rows : local * rows + window],
            allowed,
        )
        block_rows.append(masked_max(score_max, operands))
    stacked = jnp.stack(block_rows, 0)[None]
    for level in range(2):
        partner = from_partner(stacked, "seq", level)
        upper = place // (1 << level) % 2 == 1
        stacked = jnp.where(
            upper, jnp.concatenate([partner, stacked], 0), jnp.concatenate([stacked, partner], 0)
        )
    own = lax.dynamic_index_in_dim(stacked, slot, 1, False)
    row_max = own.reshape(heads, rows).T
    local_heads = jnp.max(row_max, axis=0)
    head_max = lax.pmax(local_heads, "seq")
    return finish(threshold, head_max, row_max, w_q_nope, w_q_rope, w_kv_nope)


def finish(threshold, head_max, row_max, w_q_nope, w_q_rope, w_kv_nope):
    clip = threshold[0] / jnp.maximum(head_max, threshold[0])
    root = jnp.sqrt(clip)
    new_q_nope = (w_q_nope.astype(jnp.float32) * jnp.repeat(root, D_NOPE)[None, :]).astype(
        jnp.bfloat16
    )
    new_q_rope = (w_q_rope.astype(jnp.float32) * jnp.repeat(clip, D_ROPE)[None, :]).astype(
        jnp.bfloat16
    )
    new_kv_nope = (w_kv_nope.astype(jnp.float32) * jnp.repeat(root, D_NOPE)[None, :]).astype(
        jnp.bfloat16
    )
    return (new_q_nope, new_q_rope, new_kv_nope, head_max, row_max)


MESH = pl.DeviceIdType.MESH
LANES = 128


def other(index, stride):
    return index + stride - 2 * stride * (index // stride % 2)


def gather_kernel(
    n, m, lat, rope, segs, w_nope, w_rope, w_kv,
    lat_all, rope_all, segs_all, q_cols, kv_cols,
    own_q, own_kv, lat_send, lat_recv, rope_send, rope_recv, seg_send, seg_recv,
    w_send, w_recv, local,
):
    s = lax.axis_index("seq")
    h = lax.axis_index("head")
    rows, width = lat.shape
    part = rope.shape[0]
    nope_cols = w_nope.shape[1] // n
    rope_cols = w_rope.shape[1] // n
    kv_width = w_kv.shape[1] // n
    q_rows = w_nope.shape[0]
    kv_rows = w_kv.shape[0]

    strides = []
    stride = m // 2
    while stride >= 1:
        strides.append(stride)
        stride //= 2

    barrier = pltpu.get_barrier_semaphore()
    for k in range(1, n):
        pl.semaphore_signal(barrier, inc=1, device_id=(lax.rem(s + k, n), h), device_id_type=MESH)
    for stride in strides:
        pl.semaphore_signal(barrier, inc=1, device_id=(s, other(h, stride)), device_id_type=MESH)

    mine_nope = pl.ds(pl.multiple_of(s * nope_cols, LANES), nope_cols)
    mine_rope = pl.ds(pl.multiple_of(s * rope_cols, LANES), rope_cols)
    mine_kv = pl.ds(pl.multiple_of(s * kv_width, LANES), kv_width)
    loads = [
        pltpu.make_async_copy(w_nope.at[:, mine_nope], own_q.at[:, pl.ds(0, nope_cols)], local.at[0]),
        pltpu.make_async_copy(w_rope.at[:, mine_rope], own_q.at[:, pl.ds(nope_cols, rope_cols)], local.at[1]),
        pltpu.make_async_copy(w_kv.at[:, mine_kv], own_kv, local.at[2]),
    ]
    for copy in loads:
        copy.start()

    def lat_at(ps, ph):
        return lat_all.at[pl.ds(pl.multiple_of(ps * rows, rows), rows), pl.ds(pl.multiple_of(ph * width, LANES), width)]

    def rope_at(ps, ph):
        return rope_all.at[pl.ds(pl.multiple_of((ps * m + ph) * part, part), part), :]

    stores = [
        pltpu.make_async_copy(lat, lat_at(s, h), local.at[3]),
        pltpu.make_async_copy(rope, rope_at(s, h), local.at[4]),
        pltpu.make_async_copy(segs, segs_all.at[s], local.at[5]),
    ]
    for copy in stores:
        copy.start()
    pl.semaphore_wait(barrier, n - 1 + len(strides))

    sends = []

    def piece(ps, ph, target, own):
        slot = len(sends)
        a = pltpu.make_async_remote_copy(
            src_ref=lat if own else lat_at(ps, ph), dst_ref=lat_at(ps, ph),
            send_sem=lat_send.at[slot], recv_sem=lat_recv.at[ps * m + ph],
            device_id=target, device_id_type=MESH)
        b = pltpu.make_async_remote_copy(
            src_ref=rope if own else rope_at(ps, ph), dst_ref=rope_at(ps, ph),
            send_sem=rope_send.at[slot], recv_sem=rope_recv.at[ps * m + ph],
            device_id=target, device_id_type=MESH)
        a.start()
        b.start()
        sends.append((a, b))

    def arrive(ps, ph):
        pltpu.make_async_copy(lat_at(ps, ph), lat_at(ps, ph), lat_recv.at[ps * m + ph]).wait()
        pltpu.make_async_copy(rope_at(ps, ph), rope_at(ps, ph), rope_recv.at[ps * m + ph]).wait()

    others = []

    def weights(k):
        p = lax.rem(s + k, n)
        to = (p, h)
        q_at = pl.ds(pl.multiple_of(s * q_rows, q_rows), q_rows)
        kv_at = pl.ds(pl.multiple_of(s * kv_rows, kv_rows), kv_rows)
        pairs = (
            (w_nope.at[:, pl.ds(pl.multiple_of(p * nope_cols, LANES), nope_cols)], q_cols.at[q_at, pl.ds(0, nope_cols)]),
            (w_rope.at[:, pl.ds(pl.multiple_of(p * rope_cols, LANES), rope_cols)], q_cols.at[q_at, pl.ds(nope_cols, rope_cols)]),
            (w_kv.at[:, pl.ds(pl.multiple_of(p * kv_width, LANES), kv_width)], kv_cols.at[kv_at, :]),
        )
        for i, (src, dst) in enumerate(pairs):
            copy = pltpu.make_async_remote_copy(
                src_ref=src, dst_ref=dst, send_sem=w_send.at[i * n + k], recv_sem=w_recv.at[i * n + k],
                device_id=to, device_id_type=MESH)
            copy.start()
            others.append(copy)

    pair = other(s, 1)
    even = list(range(2, n, 2))
    for k in even:
        piece(s, h, (lax.rem(s + k, n), h), True)
    piece(s, h, (pair, h), True)
    for stride in strides:
        piece(s, h, (s, other(h, stride)), True)
    for k in range(1, n):
        copy = pltpu.make_async_remote_copy(
            src_ref=segs, dst_ref=segs_all.at[s], send_sem=seg_send.at[k], recv_sem=seg_recv.at[k],
            device_id=(lax.rem(s + k, n), h), device_id_type=MESH)
        copy.start()
        others.append(copy)
    for k in even:
        weights(k)
    for k in even:
        ps = lax.rem(s + n - k, n)
        arrive(ps, h)
        piece(ps, h, (pair, h), False)
        for stride in strides:
            piece(ps, h, (s, other(h, stride)), False)
    for k in range(1, n, 2):
        weights(k)
    for copy in loads:
        copy.wait()
    keep = [
        pltpu.make_async_copy(own_q, q_cols.at[pl.ds(pl.multiple_of(s * q_rows, q_rows), q_rows), :], local.at[6]),
        pltpu.make_async_copy(own_kv, kv_cols.at[pl.ds(pl.multiple_of(s * kv_rows, kv_rows), kv_rows), :], local.at[7]),
    ]
    for copy in keep:
        copy.start()
    for k in [0] + even:
        ps = lax.rem(pair + n - k, n)
        arrive(ps, h)
        for stride in strides:
            piece(ps, h, (s, other(h, stride)), False)
    held = [h]
    for i, stride in enumerate(strides):
        fresh = [other(ph, stride) for ph in held]
        for first in range(n):
            ps = lax.rem(s + first, n)
            for ph in fresh:
                arrive(ps, ph)
                for later in strides[i + 1:]:
                    piece(ps, ph, (s, other(h, later)), False)
        held = held + fresh
    for copy in others:
        copy.wait()
    for a, b in sends:
        a.wait_send()
        b.wait_send()
    for copy in stores + keep:
        copy.wait()


def gather_all(n, m, lat, rope, segs, w_nope, w_rope, w_kv):
    rows, width = lat.shape
    part = rope.shape[0]
    q_width = (w_nope.shape[1] + w_rope.shape[1]) // n
    kv_width = w_kv.shape[1] // n
    moves = n // 2 - 1 + n * m
    any_ref = pl.BlockSpec(memory_space=pl.ANY)
    vmem = pl.BlockSpec(memory_space=pltpu.VMEM)
    dma = pltpu.SemaphoreType.DMA
    return pl.pallas_call(
        functools.partial(gather_kernel, n, m),
        out_shape=(
            jax.ShapeDtypeStruct((n * rows, m * width), lat.dtype),
            jax.ShapeDtypeStruct((n * m * part, LANES), rope.dtype),
            jax.ShapeDtypeStruct((n,) + segs.shape, segs.dtype),
            jax.ShapeDtypeStruct((n * w_nope.shape[0], q_width), w_nope.dtype),
            jax.ShapeDtypeStruct((n * w_kv.shape[0], kv_width), w_kv.dtype),
        ),
        in_specs=[vmem, vmem, vmem, any_ref, any_ref, any_ref],
        out_specs=(any_ref,) * 5,
        scratch_shapes=[
            pltpu.VMEM((w_nope.shape[0], q_width), w_nope.dtype),
            pltpu.VMEM((w_kv.shape[0], kv_width), w_kv.dtype),
            dma((moves,)), dma((n * m,)), dma((moves,)), dma((n * m,)), dma((n,)), dma((n,)),
            dma((3 * n,)), dma((3 * n,)), dma((8,)),
        ],
        compiler_params=pltpu.CompilerParams(collective_id=0, has_side_effects=True),
        name="gather_all",
    )(lat, rope, segs, w_nope, w_rope, w_kv)


def logit_kernel(m, own, q_width, lat, rope, segs, w_q, w_kv, out, keys, seg_cols):
    block = pl.program_id(0)
    rows = lat.shape[0]
    width = lat.shape[1] // m
    window = (REACH + 1) * rows
    q_lat = jnp.concatenate([lat[:, i * width : i * width + q_width] for i in range(m)], 1)
    kv_lat = jnp.concatenate([lat[:, i * width + q_width : (i + 1) * width] for i in range(m)], 1)
    q_scale = 1.0 / math.sqrt(QLORA)
    k_scale = 1.0 / math.sqrt(KVLORA)
    key = (jnp.dot(kv_lat, w_kv[...], preferred_element_type=jnp.float32) * k_scale).astype(jnp.bfloat16)
    query = (jnp.dot(q_lat, w_q[...], preferred_element_type=jnp.float32) * q_scale).astype(jnp.bfloat16)
    here = pl.ds(pl.multiple_of(block * rows, rows), rows)
    lane = lax.broadcasted_iota(jnp.int32, (rows, LANES), 1)
    twice = rope[...]
    sides = [
        jnp.where(lane // D_ROPE == side, twice, jnp.zeros_like(twice)) for side in range(LANES // D_ROPE)
    ]
    for i in range(own):
        keys[i, here, :] = jnp.concatenate(
            [key[:, i * D_NOPE : (i + 1) * D_NOPE], sides[i % len(sides)]], 1
        )
    seg_row = segs[0, 0:1, :]
    seg_cols[here, :] = jnp.transpose(jnp.broadcast_to(seg_row, (LANES, rows)))
    start = jnp.maximum(block - REACH, 0) * rows
    range_keys = pl.ds(pl.multiple_of(start, rows), window)
    key_segs = seg_cols[range_keys, :]
    key_segs = jnp.concatenate([key_segs] * (rows // LANES), 1)
    key_pos = start + lax.broadcasted_iota(jnp.int32, (window, rows), 0)
    query_pos = block * rows + lax.broadcasted_iota(jnp.int32, (window, rows), 1)
    allowed = (key_segs == seg_row) & (key_pos <= query_pos)
    base = own * D_NOPE
    found = []
    for i in range(own):
        pair = base + i // len(sides) * LANES
        q_head = jnp.concatenate(
            [query[:, i * D_NOPE : (i + 1) * D_NOPE], query[:, pair : pair + LANES]], 1
        )
        logits = lax.dot_general(
            keys[i, range_keys, :], q_head, (((1,), (1,)), ((), ())), preferred_element_type=jnp.float32
        )
        logits = jnp.where(allowed, logits, jnp.float32(-1e30))
        found.append(jnp.max(logits, axis=0, keepdims=True))
    out[0:own, here] = jnp.concatenate(found, 0) * (1.0 / math.sqrt(D_NOPE + D_ROPE))

    @pl.when(block == pl.num_programs(0) - 1)
    def _():
        top = jnp.max(out[0:own, :], axis=1, keepdims=True)
        out[own : 2 * own, :] = jnp.broadcast_to(top, (own, out.shape[1]))


def logit_maxima(n, m, own, q_width, lat, rope, segs, w_q, w_kv):
    rows = lat.shape[0] // n
    return pl.pallas_call(
        functools.partial(logit_kernel, m, own, q_width),
        grid=(n,),
        out_shape=jax.ShapeDtypeStruct((2 * own, lat.shape[0]), jnp.float32),
        in_specs=[
            pl.BlockSpec((rows, lat.shape[1]), lambda i: (i, 0)),
            pl.BlockSpec((rows, LANES), lambda i: (i, 0)),
            pl.BlockSpec((1,) + segs.shape[1:], lambda i: (i, 0, 0)),
            pl.BlockSpec(w_q.shape, lambda i: (0, 0)),
            pl.BlockSpec(w_kv.shape, lambda i: (0, 0)),
        ],
        out_specs=pl.BlockSpec((2 * own, lat.shape[0]), lambda i: (0, 0)),
        scratch_shapes=[
            pltpu.VMEM((own, lat.shape[0], D_NOPE + LANES), jnp.bfloat16),
            pltpu.VMEM((lat.shape[0], LANES), jnp.int32),
        ],
        compiler_params=pltpu.CompilerParams(dimension_semantics=("arbitrary",)),
        name="logit_maxima",
    )(lat, rope, segs, w_q, w_kv)


def exchange_kernel(n, maxima, out, send, recv):
    s = lax.axis_index("seq")
    h = lax.axis_index("head")
    rows = out.shape[2]
    barrier = pltpu.get_barrier_semaphore()
    for k in range(1, n):
        pl.semaphore_signal(barrier, inc=1, device_id=(lax.rem(s + k, n), h), device_id_type=MESH)
    pl.semaphore_wait(barrier, n - 1)
    copies = []
    for k in range(1, n):
        p = lax.rem(s + k, n)
        copy = pltpu.make_async_remote_copy(
            src_ref=maxima.at[:, pl.ds(pl.multiple_of(p * rows, rows), rows)], dst_ref=out.at[s],
            send_sem=send.at[k], recv_sem=recv.at[k], device_id=(p, h), device_id_type=MESH)
        copy.start()
        copies.append(copy)
    out[s] = maxima[:, pl.ds(pl.multiple_of(s * rows, rows), rows)]
    for copy in copies:
        copy.wait()


def exchange(n, maxima):
    vmem = pl.BlockSpec(memory_space=pltpu.VMEM)
    return pl.pallas_call(
        functools.partial(exchange_kernel, n),
        out_shape=jax.ShapeDtypeStruct((n, maxima.shape[0], maxima.shape[1] // n), jnp.float32),
        in_specs=[vmem],
        out_specs=vmem,
        scratch_shapes=[pltpu.SemaphoreType.DMA((n,)), pltpu.SemaphoreType.DMA((n,))],
        compiler_params=pltpu.CompilerParams(collective_id=1, has_side_effects=True),
        name="exchange",
    )(maxima)


def owned_body(n, m, q_latent, kv_latent, k_rope, segment_ids, w_q_nope, w_q_rope, w_kv_nope, threshold):
    rows, q_width = q_latent.shape
    heads = w_q_nope.shape[1] // D_NOPE
    own = heads // n
    lat = jnp.concatenate([q_latent, kv_latent], 1)
    part = rows // m
    rope = lax.dynamic_slice_in_dim(k_rope, lax.axis_index("head") * part, part, 0)
    rope = jnp.concatenate([rope] * (LANES // D_ROPE), 1)
    segs = jnp.broadcast_to(segment_ids[None], (8, rows))
    lat_all, rope_all, segs_all, w_q, w_kv = gather_all(n, m, lat, rope, segs, w_q_nope, w_q_rope, w_kv_nope)
    maxima = logit_maxima(n, m, own, q_width, lat_all, rope_all, segs_all, w_q, w_kv)
    got = exchange(n, maxima)
    row_max = got[:, :own, :].reshape(heads, rows).T
    head_max = got[:, own:, 0].reshape(heads)
    return finish(threshold, head_max, row_max, w_q_nope, w_q_rope, w_kv_nope)


def body(n, m, *operands):
    heads = operands[4].shape[1] // D_NOPE
    rows = operands[0].shape[0]
    shares = heads % n == 0 and heads // n % (LANES // D_ROPE) == 0
    fits = n % 2 == 0 and n > REACH and m & (m - 1) == 0 and rows % LANES == 0 and rows // m % 16 == 0
    if shares and fits and heads // n % 4 == 0:
        return owned_body(n, m, *operands)
    return grouped_body(*operands)


def solution(mesh):
    in_specs = (
        P("seq", "head"),
        P("seq", "head"),
        P("seq", None),
        P("seq"),
        P("seq", "head"),
        P("seq", "head"),
        P("seq", "head"),
        P(),
    )
    out_specs = (P("seq", "head"), P("seq", "head"), P("seq", "head"), P("head"), P("seq", "head"))
    return jax.shard_map(functools.partial(body, mesh.shape["seq"], mesh.shape["head"]), mesh=mesh, in_specs=in_specs, out_specs=out_specs, check_vma=False)
```

```python
import functools
import math

import jax
import jax.numpy as jnp
from jax import lax
from jax.experimental import pallas as pl
from jax.experimental.pallas import tpu as pltpu
from jax.sharding import PartitionSpec as P

D_NOPE = 128
D_ROPE = 64
QLORA = 1536
KVLORA = 512
REACH = 3


def as_sent(value):
    return jax.tree.map(lambda a: a.astype(jnp.bfloat16) if a.dtype == jnp.float32 else a, value)


def from_partner(value, axis, stride):
    mask = 2**stride
    pairs = [(source, source ^ mask) for source in range(lax.axis_size(axis))]
    return lax.ppermute(value, axis, pairs)


def shifted(block, axis, distance):
    devices = range(lax.axis_size(axis))
    route = [(i - distance, i) for i in devices if i - distance in devices]
    return lax.ppermute(block, axis, route)


def score_max(query_nope, query_rope, key_nope, key_rope, allowed):
    nope = jnp.einsum("qhd,khd->hqk", query_nope, key_nope, preferred_element_type=jnp.float32)
    rope = jnp.einsum("qhd,kd->hqk", query_rope, key_rope, preferred_element_type=jnp.float32)
    scores = (nope + rope) * (1.0 / math.sqrt(D_NOPE + D_ROPE))
    return jnp.max(jnp.where(allowed[None], scores, jnp.float32(-1e30)), axis=2)


def masked_max(compute, operands):
    return compute(*operands)


def spread_columns(weight, width, quarter, copies):
    pieces = weight.reshape(weight.shape[0], 4, quarter * width).transpose(1, 0, 2)
    return jnp.tile(pieces, (copies, 1, 1))


def grouped_body(q_latent, kv_latent, k_rope, segment_ids, w_q_nope, w_q_rope, w_kv_nope, threshold):
    q_whole, kv_whole = (
        lax.all_gather(q_latent, "head", axis=1, tiled=True),
        lax.all_gather(kv_latent, "head", axis=1, tiled=True),
    )
    rows = q_whole.shape[0]
    heads = w_q_nope.shape[1] // D_NOPE
    q_scale = 1.0 / math.sqrt(QLORA)
    k_scale = 1.0 / math.sqrt(KVLORA)
    place = lax.axis_index("seq")
    quarter = heads // 4
    copies = lax.axis_size("seq") // 4
    slot = place % 4
    sent = (
        spread_columns(w_q_nope, D_NOPE, quarter, copies),
        spread_columns(w_q_rope, D_ROPE, quarter, copies),
        spread_columns(w_kv_nope, D_NOPE, quarter, copies),
    )
    got_nope, got_rope, got_kv = (
        lax.all_to_all(sent[0], "seq", split_axis=0, concat_axis=1, tiled=True),
        lax.all_to_all(sent[1], "seq", split_axis=0, concat_axis=1, tiled=True),
        lax.all_to_all(sent[2], "seq", split_axis=0, concat_axis=1, tiled=True),
    )
    sub_nope = got_nope.reshape(QLORA, quarter * D_NOPE)
    sub_rope = got_rope.reshape(QLORA, quarter * D_ROPE)
    sub_kv = got_kv.reshape(KVLORA, quarter * D_NOPE)
    group = (q_whole, kv_whole, k_rope)
    for level in range(2):
        partner = jax.tree.map(
            lambda part, own: part.astype(own.dtype),
            from_partner(as_sent(group), "seq", level),
            group,
        )
        upper = place // (1 << level) % 2 == 1
        group = tuple(
            (
                jnp.where(
                    upper, jnp.concatenate([other, mine], 0), jnp.concatenate([mine, other], 0)
                )
                for mine, other in zip(group, partner)
            )
        )
    group_q, group_kv, group_rope = group
    early_kv, early_rope = shifted(
        (group_kv[(4 - REACH) * rows :], group_rope[(4 - REACH) * rows :]), "seq", 4
    )
    keys_kv = jnp.concatenate([early_kv, group_kv], 0)
    keys_rope = jnp.concatenate([early_rope, group_rope], 0)
    key_nope = (
        (jnp.dot(keys_kv, sub_kv, preferred_element_type=jnp.float32) * k_scale)
        .astype(jnp.bfloat16)
        .reshape(keys_kv.shape[0], quarter, D_NOPE)
    )
    query_nope = (
        (jnp.dot(group_q, sub_nope, preferred_element_type=jnp.float32) * q_scale)
        .astype(jnp.bfloat16)
        .reshape(4 * rows, quarter, D_NOPE)
    )
    query_rope = (
        (jnp.dot(group_q, sub_rope, preferred_element_type=jnp.float32) * q_scale)
        .astype(jnp.bfloat16)
        .reshape(4 * rows, quarter, D_ROPE)
    )
    all_segs = lax.all_gather(segment_ids, "seq", axis=0, tiled=True)
    padded_segs = jnp.concatenate([jnp.full((REACH * rows,), -1, jnp.int32), all_segs], 0)
    first = place // 4 * 4
    window = (REACH + 1) * rows
    block_rows = []
    for local in range(4):
        block = first + local
        query_seg = lax.dynamic_slice_in_dim(all_segs, block * rows, rows, 0)
        key_seg = lax.dynamic_slice_in_dim(padded_segs, block * rows, window, 0)
        query_pos = block * rows + jnp.arange(rows, dtype=jnp.int32)
        key_pos = (block - REACH) * rows + jnp.arange(window, dtype=jnp.int32)
        allowed = (
            (query_seg[:, None] == key_seg[None, :])
            & (key_pos[None, :] <= query_pos[:, None])
            & (key_pos[None, :] >= 0)
        )
        operands = (
            query_nope[local * rows : (local + 1) * rows],
            query_rope[local * rows : (local + 1) * rows],
            key_nope[local * rows : local * rows + window],
            keys_rope[local * rows : local * rows + window],
            allowed,
        )
        block_rows.append(masked_max(score_max, operands))
    stacked = jnp.stack(block_rows, 0)[None]
    for level in range(2):
        partner = from_partner(stacked, "seq", level)
        upper = place // (1 << level) % 2 == 1
        stacked = jnp.where(
            upper, jnp.concatenate([partner, stacked], 0), jnp.concatenate([stacked, partner], 0)
        )
    own = lax.dynamic_index_in_dim(stacked, slot, 1, False)
    row_max = own.reshape(heads, rows).T
    local_heads = jnp.max(row_max, axis=0)
    head_max = lax.pmax(local_heads, "seq")
    return finish(threshold, head_max, row_max, w_q_nope, w_q_rope, w_kv_nope)


def finish(threshold, head_max, row_max, w_q_nope, w_q_rope, w_kv_nope):
    clip = threshold[0] / jnp.maximum(head_max, threshold[0])
    root = jnp.sqrt(clip)
    new_q_nope = (w_q_nope.astype(jnp.float32) * jnp.repeat(root, D_NOPE)[None, :]).astype(
        jnp.bfloat16
    )
    new_q_rope = (w_q_rope.astype(jnp.float32) * jnp.repeat(clip, D_ROPE)[None, :]).astype(
        jnp.bfloat16
    )
    new_kv_nope = (w_kv_nope.astype(jnp.float32) * jnp.repeat(root, D_NOPE)[None, :]).astype(
        jnp.bfloat16
    )
    return (new_q_nope, new_q_rope, new_kv_nope, head_max, row_max)


MESH = pl.DeviceIdType.MESH
LANES = 128


def other(index, stride):
    return index + stride - 2 * stride * (index // stride % 2)


def gather_kernel(
    n, m, q_lat, kv_lat, rope, segs, w_nope, w_rope, w_kv,
    q_all, kv_all, rope_all, segs_all, q_cols, kv_cols,
    own_q, own_kv, q_send, q_recv, kv_send, kv_recv, rope_send, rope_recv, seg_send, seg_recv,
    w_send, w_recv, local,
):
    s = lax.axis_index("seq")
    h = lax.axis_index("head")
    rows = q_lat.shape[0]
    part = rope.shape[0] // m
    nope_cols = w_nope.shape[1] // n
    rope_cols = w_rope.shape[1] // n
    kv_width = w_kv.shape[1] // n
    q_rows = w_nope.shape[0]
    kv_rows = w_kv.shape[0]

    strides = []
    stride = m // 2
    while stride >= 1:
        strides.append(stride)
        stride //= 2

    barrier = pltpu.get_barrier_semaphore()
    for k in range(1, n):
        pl.semaphore_signal(barrier, inc=1, device_id=(lax.rem(s + k, n), h), device_id_type=MESH)
    for stride in strides:
        pl.semaphore_signal(barrier, inc=1, device_id=(s, other(h, stride)), device_id_type=MESH)

    mine_nope = pl.ds(pl.multiple_of(s * nope_cols, LANES), nope_cols)
    mine_rope = pl.ds(pl.multiple_of(s * rope_cols, LANES), rope_cols)
    mine_kv = pl.ds(pl.multiple_of(s * kv_width, LANES), kv_width)
    loads = [
        pltpu.make_async_copy(w_nope.at[:, mine_nope], own_q.at[:, pl.ds(0, nope_cols)], local.at[0]),
        pltpu.make_async_copy(w_rope.at[:, mine_rope], own_q.at[:, pl.ds(nope_cols, rope_cols)], local.at[1]),
        pltpu.make_async_copy(w_kv.at[:, mine_kv], own_kv, local.at[2]),
    ]
    for copy in loads:
        copy.start()

    def window(whole, lat, ps, ph):
        width = lat.shape[1]
        return whole.at[pl.ds(pl.multiple_of(ps * rows, rows), rows), pl.ds(pl.multiple_of(ph * width, LANES), width)]

    def rope_at(ps, ph):
        return rope_all.at[ps, pl.ds(pl.multiple_of(ph * part, part), part), :]

    def places(ps, ph):
        return window(q_all, q_lat, ps, ph), window(kv_all, kv_lat, ps, ph), rope_at(ps, ph)

    mine = (q_lat, kv_lat, rope.at[pl.ds(pl.multiple_of(h * part, part), part), :])
    send_sems = (q_send, kv_send, rope_send)
    recv_sems = (q_recv, kv_recv, rope_recv)
    stores = [
        pltpu.make_async_copy(src, dst, local.at[3 + i])
        for i, (src, dst) in enumerate(zip(mine + (segs,), places(s, h) + (segs_all.at[s],)))
    ]
    for copy in stores:
        copy.start()
    pl.semaphore_wait(barrier, n - 1 + len(strides))

    sends = []
    slots = [0]

    def piece(ps, ph, target, own, when=None):
        slot = slots[0]
        slots[0] += 1
        copies = [
            pltpu.make_async_remote_copy(
                src_ref=src, dst_ref=dst, send_sem=sent.at[slot], recv_sem=got.at[ps * m + ph],
                device_id=target, device_id_type=MESH)
            for src, dst, sent, got in zip(
                mine if own else places(ps, ph), places(ps, ph), send_sems, recv_sems)
        ]
        for copy in copies:
            copy.start()

        def drain():
            for sent, src in zip(send_sems, mine):
                pltpu.make_async_copy(src, src, sent.at[slot]).wait()

        sends.append((when, drain))

    def arrive(ps, ph):
        for at, got in zip(places(ps, ph), recv_sems):
            pltpu.make_async_copy(at, at, got.at[ps * m + ph]).wait()

    others = []

    def weights(k):
        p = lax.rem(s + k, n)
        to = (p, h)
        q_at = pl.ds(pl.multiple_of(s * q_rows, q_rows), q_rows)
        kv_at = pl.ds(pl.multiple_of(s * kv_rows, kv_rows), kv_rows)
        pairs = (
            (w_nope.at[:, pl.ds(pl.multiple_of(p * nope_cols, LANES), nope_cols)], q_cols.at[q_at, pl.ds(0, nope_cols)]),
            (w_rope.at[:, pl.ds(pl.multiple_of(p * rope_cols, LANES), rope_cols)], q_cols.at[q_at, pl.ds(nope_cols, rope_cols)]),
            (w_kv.at[:, pl.ds(pl.multiple_of(p * kv_width, LANES), kv_width)], kv_cols.at[kv_at, :]),
        )
        for i, (src, dst) in enumerate(pairs):
            copy = pltpu.make_async_remote_copy(
                src_ref=src, dst_ref=dst, send_sem=w_send.at[i * n + k], recv_sem=w_recv.at[i * n + k],
                device_id=to, device_id_type=MESH)
            copy.start()
            others.append(copy)

    pair = other(s, 1)
    even = list(range(2, n, 2))

    def inside(index):
        return (index >= 0) & (index < n)

    for sign in (-2, 2):
        @pl.when(inside(s + sign))
        def _(sign=sign):
            piece(s, h, (s + sign, h), True, lambda: inside(s + sign))
    piece(s, h, (pair, h), True)
    for stride in strides:
        piece(s, h, (s, other(h, stride)), True)
    for step in range(1, n // 2):
        for sign in (-2, 2):
            ps = s + sign * step
            ahead = s - sign

            @pl.when(inside(ps) & inside(ahead))
            def _(ps=ps, ahead=ahead):
                arrive(ps, h)
                piece(ps, h, (ahead, h), False, lambda: inside(ps) & inside(ahead))

            @pl.when(inside(ps) & (ahead < 0) | inside(ps) & (ahead >= n))
            def _(ps=ps):
                arrive(ps, h)

            @pl.when(inside(ps))
            def _(ps=ps):
                piece(ps, h, (pair, h), False, lambda: inside(ps))
                for stride in strides:
                    piece(ps, h, (s, other(h, stride)), False, lambda: inside(ps))
        if step == 1:
            for k in range(1, n):
                copy = pltpu.make_async_remote_copy(
                    src_ref=segs, dst_ref=segs_all.at[s], send_sem=seg_send.at[k], recv_sem=seg_recv.at[k],
                    device_id=(lax.rem(s + k, n), h), device_id_type=MESH)
                copy.start()
                others.append(copy)
            for k in even:
                weights(k)
    for k in range(1, n, 2):
        weights(k)
    for copy in loads:
        copy.wait()
    keep = [
        pltpu.make_async_copy(own_q, q_cols.at[pl.ds(pl.multiple_of(s * q_rows, q_rows), q_rows), :], local.at[7]),
        pltpu.make_async_copy(own_kv, kv_cols.at[pl.ds(pl.multiple_of(s * kv_rows, kv_rows), kv_rows), :], local.at[8]),
    ]
    for copy in keep:
        copy.start()
    for k in [0] + even:
        ps = lax.rem(pair + n - k, n)
        arrive(ps, h)
        for stride in strides:
            piece(ps, h, (s, other(h, stride)), False)
    held = [h]
    for i, stride in enumerate(strides):
        fresh = [other(ph, stride) for ph in held]
        for first in range(n):
            ps = lax.rem(s + first, n)
            for ph in fresh:
                arrive(ps, ph)
                for later in strides[i + 1:]:
                    piece(ps, ph, (s, other(h, later)), False)
        held = held + fresh
    for copy in others:
        copy.wait()
    for when, drain in sends:
        if when is None:
            drain()
        else:
            pl.when(when())(drain)
    for copy in stores + keep:
        copy.wait()


def gather_all(n, m, q_lat, kv_lat, rope, segs, w_nope, w_rope, w_kv):
    rows = q_lat.shape[0]
    q_width = (w_nope.shape[1] + w_rope.shape[1]) // n
    kv_width = w_kv.shape[1] // n
    moves = 2 + 2 * (n // 2 - 1) + (n - 1) * (m + 1) + n * m
    any_ref = pl.BlockSpec(memory_space=pl.ANY)
    vmem = pl.BlockSpec(memory_space=pltpu.VMEM)
    dma = pltpu.SemaphoreType.DMA
    return pl.pallas_call(
        functools.partial(gather_kernel, n, m),
        out_shape=(
            jax.ShapeDtypeStruct((n * rows, m * q_lat.shape[1]), q_lat.dtype),
            jax.ShapeDtypeStruct((n * rows, m * kv_lat.shape[1]), kv_lat.dtype),
            jax.ShapeDtypeStruct((n,) + rope.shape, rope.dtype),
            jax.ShapeDtypeStruct((n,) + segs.shape, segs.dtype),
            jax.ShapeDtypeStruct((n * w_nope.shape[0], q_width), w_nope.dtype),
            jax.ShapeDtypeStruct((n * w_kv.shape[0], kv_width), w_kv.dtype),
        ),
        in_specs=[vmem, vmem, vmem, vmem, any_ref, any_ref, any_ref],
        out_specs=(any_ref,) * 6,
        scratch_shapes=[
            pltpu.VMEM((w_nope.shape[0], q_width), w_nope.dtype),
            pltpu.VMEM((w_kv.shape[0], kv_width), w_kv.dtype),
            dma((moves,)), dma((n * m,)), dma((moves,)), dma((n * m,)), dma((moves,)), dma((n * m,)),
            dma((n,)), dma((n,)),
            dma((3 * n,)), dma((3 * n,)), dma((9,)),
        ],
        compiler_params=pltpu.CompilerParams(collective_id=0, has_side_effects=True),
        name="gather_all",
    )(q_lat, kv_lat, rope, segs, w_nope, w_rope, w_kv)


def logit_kernel(own, q_lat, kv_lat, rope, segs, w_q, w_kv, out, keys, seg_cols):
    block = pl.program_id(0)
    rows = q_lat.shape[0]
    window = (REACH + 1) * rows
    q_scale = 1.0 / math.sqrt(QLORA)
    k_scale = 1.0 / math.sqrt(KVLORA)
    key = (jnp.dot(kv_lat[...], w_kv[...], preferred_element_type=jnp.float32) * k_scale).astype(jnp.bfloat16)
    query = (jnp.dot(q_lat[...], w_q[...], preferred_element_type=jnp.float32) * q_scale).astype(jnp.bfloat16)
    here = pl.ds(pl.multiple_of(block * rows, rows), rows)
    lane = lax.broadcasted_iota(jnp.int32, (rows, LANES), 1)
    turned = jnp.concatenate([rope[0].astype(jnp.float32)] * (LANES // D_ROPE), 0)
    twice = jnp.transpose(turned).astype(jnp.bfloat16)
    sides = [
        jnp.where(lane // D_ROPE == side, twice, jnp.zeros_like(twice)) for side in range(LANES // D_ROPE)
    ]
    for i in range(own):
        keys[i, here, :] = jnp.concatenate(
            [key[:, i * D_NOPE : (i + 1) * D_NOPE], sides[i % len(sides)]], 1
        )
    seg_row = segs[0]
    seg_cols[here, :] = jnp.transpose(jnp.broadcast_to(seg_row, (LANES, rows)))
    start = jnp.maximum(block - REACH, 0) * rows
    range_keys = pl.ds(pl.multiple_of(start, rows), window)
    key_segs = seg_cols[range_keys, :]
    key_segs = jnp.concatenate([key_segs] * (rows // LANES), 1)
    key_pos = start + lax.broadcasted_iota(jnp.int32, (window, rows), 0)
    query_pos = block * rows + lax.broadcasted_iota(jnp.int32, (window, rows), 1)
    allowed = (key_segs == seg_row) & (key_pos <= query_pos)
    base = own * D_NOPE
    found = []
    for i in range(own):
        pair = base + i // len(sides) * LANES
        q_head = jnp.concatenate(
            [query[:, i * D_NOPE : (i + 1) * D_NOPE], query[:, pair : pair + LANES]], 1
        )
        logits = lax.dot_general(
            keys[i, range_keys, :], q_head, (((1,), (1,)), ((), ())), preferred_element_type=jnp.float32
        )
        logits = jnp.where(allowed, logits, jnp.float32(-1e30))
        found.append(jnp.max(logits, axis=0, keepdims=True))
    out[0:own, here] = jnp.concatenate(found, 0) * (1.0 / math.sqrt(D_NOPE + D_ROPE))

    @pl.when(block == pl.num_programs(0) - 1)
    def _():
        top = jnp.max(out[0:own, :], axis=1, keepdims=True)
        out[own : 2 * own, :] = jnp.broadcast_to(top, (own, out.shape[1]))


def logit_maxima(n, own, q_lat, kv_lat, rope, segs, w_q, w_kv):
    rows = q_lat.shape[0] // n
    return pl.pallas_call(
        functools.partial(logit_kernel, own),
        grid=(n,),
        out_shape=jax.ShapeDtypeStruct((2 * own, q_lat.shape[0]), jnp.float32),
        in_specs=[
            pl.BlockSpec((rows, q_lat.shape[1]), lambda i: (i, 0)),
            pl.BlockSpec((rows, kv_lat.shape[1]), lambda i: (i, 0)),
            pl.BlockSpec((1,) + rope.shape[1:], lambda i: (i, 0, 0)),
            pl.BlockSpec((1,) + segs.shape[1:], lambda i: (i, 0, 0)),
            pl.BlockSpec(w_q.shape, lambda i: (0, 0)),
            pl.BlockSpec(w_kv.shape, lambda i: (0, 0)),
        ],
        out_specs=pl.BlockSpec((2 * own, q_lat.shape[0]), lambda i: (0, 0)),
        scratch_shapes=[
            pltpu.VMEM((own, q_lat.shape[0], D_NOPE + LANES), jnp.bfloat16),
            pltpu.VMEM((q_lat.shape[0], LANES), jnp.int32),
        ],
        compiler_params=pltpu.CompilerParams(dimension_semantics=("arbitrary",)),
        name="logit_maxima",
    )(q_lat, kv_lat, rope, segs, w_q, w_kv)


def exchange_kernel(n, maxima, out, send, recv):
    s = lax.axis_index("seq")
    h = lax.axis_index("head")
    rows = out.shape[2]
    barrier = pltpu.get_barrier_semaphore()
    for k in range(1, n):
        pl.semaphore_signal(barrier, inc=1, device_id=(lax.rem(s + k, n), h), device_id_type=MESH)
    pl.semaphore_wait(barrier, n - 1)
    copies = []
    for k in range(1, n):
        p = lax.rem(s + k, n)
        copy = pltpu.make_async_remote_copy(
            src_ref=maxima.at[:, pl.ds(pl.multiple_of(p * rows, rows), rows)], dst_ref=out.at[s],
            send_sem=send.at[k], recv_sem=recv.at[k], device_id=(p, h), device_id_type=MESH)
        copy.start()
        copies.append(copy)
    out[s] = maxima[:, pl.ds(pl.multiple_of(s * rows, rows), rows)]
    for copy in copies:
        copy.wait()


def exchange(n, maxima):
    vmem = pl.BlockSpec(memory_space=pltpu.VMEM)
    return pl.pallas_call(
        functools.partial(exchange_kernel, n),
        out_shape=jax.ShapeDtypeStruct((n, maxima.shape[0], maxima.shape[1] // n), jnp.float32),
        in_specs=[vmem],
        out_specs=vmem,
        scratch_shapes=[pltpu.SemaphoreType.DMA((n,)), pltpu.SemaphoreType.DMA((n,))],
        compiler_params=pltpu.CompilerParams(collective_id=1, has_side_effects=True),
        name="exchange",
    )(maxima)


def owned_body(n, m, q_latent, kv_latent, k_rope, segment_ids, w_q_nope, w_q_rope, w_kv_nope, threshold):
    rows = q_latent.shape[0]
    heads = w_q_nope.shape[1] // D_NOPE
    own = heads // n
    gathered = gather_all(
        n, m, q_latent, kv_latent, k_rope.T, segment_ids.reshape(1, rows), w_q_nope, w_q_rope, w_kv_nope
    )
    maxima = logit_maxima(n, own, *gathered)
    got = exchange(n, maxima)
    row_max = got[:, :own, :].reshape(heads, rows).T
    head_max = got[:, own:, 0].reshape(heads)
    return finish(threshold, head_max, row_max, w_q_nope, w_q_rope, w_kv_nope)


def body(n, m, *operands):
    heads = operands[4].shape[1] // D_NOPE
    rows = operands[0].shape[0]
    shares = heads % n == 0 and heads // n % (LANES // D_ROPE) == 0
    fits = n % 2 == 0 and n > REACH and m & (m - 1) == 0 and rows % LANES == 0 and operands[2].shape[1] % (16 * m) == 0
    if shares and fits and heads // n % 4 == 0:
        return owned_body(n, m, *operands)
    return grouped_body(*operands)


def solution(mesh):
    in_specs = (
        P("seq", "head"),
        P("seq", "head"),
        P("seq", None),
        P("seq"),
        P("seq", "head"),
        P("seq", "head"),
        P("seq", "head"),
        P(),
    )
    out_specs = (P("seq", "head"), P("seq", "head"), P("seq", "head"), P("head"), P("seq", "head"))
    return jax.shard_map(functools.partial(body, mesh.shape["seq"], mesh.shape["head"]), mesh=mesh, in_specs=in_specs, out_specs=out_specs, check_vma=False)
```

```python
import functools
import math

import jax
import jax.numpy as jnp
from jax import lax
from jax.experimental import pallas as pl
from jax.experimental.pallas import tpu as pltpu
from jax.sharding import PartitionSpec as P

D_NOPE = 128
D_ROPE = 64
QLORA = 1536
KVLORA = 512
REACH = 3


def as_sent(value):
    return jax.tree.map(lambda a: a.astype(jnp.bfloat16) if a.dtype == jnp.float32 else a, value)


def from_partner(value, axis, stride):
    mask = 2**stride
    pairs = [(source, source ^ mask) for source in range(lax.axis_size(axis))]
    return lax.ppermute(value, axis, pairs)


def shifted(block, axis, distance):
    devices = range(lax.axis_size(axis))
    route = [(i - distance, i) for i in devices if i - distance in devices]
    return lax.ppermute(block, axis, route)


def score_max(query_nope, query_rope, key_nope, key_rope, allowed):
    nope = jnp.einsum("qhd,khd->hqk", query_nope, key_nope, preferred_element_type=jnp.float32)
    rope = jnp.einsum("qhd,kd->hqk", query_rope, key_rope, preferred_element_type=jnp.float32)
    scores = (nope + rope) * (1.0 / math.sqrt(D_NOPE + D_ROPE))
    return jnp.max(jnp.where(allowed[None], scores, jnp.float32(-1e30)), axis=2)


def masked_max(compute, operands):
    return compute(*operands)


def spread_columns(weight, width, quarter, copies):
    pieces = weight.reshape(weight.shape[0], 4, quarter * width).transpose(1, 0, 2)
    return jnp.tile(pieces, (copies, 1, 1))


def grouped_body(q_latent, kv_latent, k_rope, segment_ids, w_q_nope, w_q_rope, w_kv_nope, threshold):
    q_whole, kv_whole = (
        lax.all_gather(q_latent, "head", axis=1, tiled=True),
        lax.all_gather(kv_latent, "head", axis=1, tiled=True),
    )
    rows = q_whole.shape[0]
    heads = w_q_nope.shape[1] // D_NOPE
    q_scale = 1.0 / math.sqrt(QLORA)
    k_scale = 1.0 / math.sqrt(KVLORA)
    place = lax.axis_index("seq")
    quarter = heads // 4
    copies = lax.axis_size("seq") // 4
    slot = place % 4
    sent = (
        spread_columns(w_q_nope, D_NOPE, quarter, copies),
        spread_columns(w_q_rope, D_ROPE, quarter, copies),
        spread_columns(w_kv_nope, D_NOPE, quarter, copies),
    )
    got_nope, got_rope, got_kv = (
        lax.all_to_all(sent[0], "seq", split_axis=0, concat_axis=1, tiled=True),
        lax.all_to_all(sent[1], "seq", split_axis=0, concat_axis=1, tiled=True),
        lax.all_to_all(sent[2], "seq", split_axis=0, concat_axis=1, tiled=True),
    )
    sub_nope = got_nope.reshape(QLORA, quarter * D_NOPE)
    sub_rope = got_rope.reshape(QLORA, quarter * D_ROPE)
    sub_kv = got_kv.reshape(KVLORA, quarter * D_NOPE)
    group = (q_whole, kv_whole, k_rope)
    for level in range(2):
        partner = jax.tree.map(
            lambda part, own: part.astype(own.dtype),
            from_partner(as_sent(group), "seq", level),
            group,
        )
        upper = place // (1 << level) % 2 == 1
        group = tuple(
            (
                jnp.where(
                    upper, jnp.concatenate([other, mine], 0), jnp.concatenate([mine, other], 0)
                )
                for mine, other in zip(group, partner)
            )
        )
    group_q, group_kv, group_rope = group
    early_kv, early_rope = shifted(
        (group_kv[(4 - REACH) * rows :], group_rope[(4 - REACH) * rows :]), "seq", 4
    )
    keys_kv = jnp.concatenate([early_kv, group_kv], 0)
    keys_rope = jnp.concatenate([early_rope, group_rope], 0)
    key_nope = (
        (jnp.dot(keys_kv, sub_kv, preferred_element_type=jnp.float32) * k_scale)
        .astype(jnp.bfloat16)
        .reshape(keys_kv.shape[0], quarter, D_NOPE)
    )
    query_nope = (
        (jnp.dot(group_q, sub_nope, preferred_element_type=jnp.float32) * q_scale)
        .astype(jnp.bfloat16)
        .reshape(4 * rows, quarter, D_NOPE)
    )
    query_rope = (
        (jnp.dot(group_q, sub_rope, preferred_element_type=jnp.float32) * q_scale)
        .astype(jnp.bfloat16)
        .reshape(4 * rows, quarter, D_ROPE)
    )
    all_segs = lax.all_gather(segment_ids, "seq", axis=0, tiled=True)
    padded_segs = jnp.concatenate([jnp.full((REACH * rows,), -1, jnp.int32), all_segs], 0)
    first = place // 4 * 4
    window = (REACH + 1) * rows
    block_rows = []
    for local in range(4):
        block = first + local
        query_seg = lax.dynamic_slice_in_dim(all_segs, block * rows, rows, 0)
        key_seg = lax.dynamic_slice_in_dim(padded_segs, block * rows, window, 0)
        query_pos = block * rows + jnp.arange(rows, dtype=jnp.int32)
        key_pos = (block - REACH) * rows + jnp.arange(window, dtype=jnp.int32)
        allowed = (
            (query_seg[:, None] == key_seg[None, :])
            & (key_pos[None, :] <= query_pos[:, None])
            & (key_pos[None, :] >= 0)
        )
        operands = (
            query_nope[local * rows : (local + 1) * rows],
            query_rope[local * rows : (local + 1) * rows],
            key_nope[local * rows : local * rows + window],
            keys_rope[local * rows : local * rows + window],
            allowed,
        )
        block_rows.append(masked_max(score_max, operands))
    stacked = jnp.stack(block_rows, 0)[None]
    for level in range(2):
        partner = from_partner(stacked, "seq", level)
        upper = place // (1 << level) % 2 == 1
        stacked = jnp.where(
            upper, jnp.concatenate([partner, stacked], 0), jnp.concatenate([stacked, partner], 0)
        )
    own = lax.dynamic_index_in_dim(stacked, slot, 1, False)
    row_max = own.reshape(heads, rows).T
    local_heads = jnp.max(row_max, axis=0)
    head_max = lax.pmax(local_heads, "seq")
    return finish(threshold, head_max, row_max, w_q_nope, w_q_rope, w_kv_nope)


def finish(threshold, head_max, row_max, w_q_nope, w_q_rope, w_kv_nope):
    clip = threshold[0] / jnp.maximum(head_max, threshold[0])
    root = jnp.sqrt(clip)
    new_q_nope = (w_q_nope.astype(jnp.float32) * jnp.repeat(root, D_NOPE)[None, :]).astype(
        jnp.bfloat16
    )
    new_q_rope = (w_q_rope.astype(jnp.float32) * jnp.repeat(clip, D_ROPE)[None, :]).astype(
        jnp.bfloat16
    )
    new_kv_nope = (w_kv_nope.astype(jnp.float32) * jnp.repeat(root, D_NOPE)[None, :]).astype(
        jnp.bfloat16
    )
    return (new_q_nope, new_q_rope, new_kv_nope, head_max, row_max)


MESH = pl.DeviceIdType.MESH
LANES = 128


def other(index, stride):
    return index + stride - 2 * stride * (index // stride % 2)


def gather_kernel(
    n, m, q_lat, kv_lat, rope, segs, w_nope, w_rope, w_kv,
    q_all, kv_all, rope_all, segs_all, q_cols, kv_cols,
    own_q, own_kv, q_send, q_recv, kv_send, kv_recv, rope_send, rope_recv, seg_send, seg_recv,
    w_send, w_recv, local,
):
    s = lax.axis_index("seq")
    h = lax.axis_index("head")
    rows = q_lat.shape[0]
    part = rope.shape[0] // m
    nope_cols = w_nope.shape[1] // n
    rope_cols = w_rope.shape[1] // n
    kv_width = w_kv.shape[1] // n
    q_rows = w_nope.shape[0]
    kv_rows = w_kv.shape[0]

    strides = []
    stride = m // 2
    while stride >= 1:
        strides.append(stride)
        stride //= 2

    barrier = pltpu.get_barrier_semaphore()
    for k in range(1, n):
        pl.semaphore_signal(barrier, inc=1, device_id=(lax.rem(s + k, n), h), device_id_type=MESH)
    for stride in strides:
        pl.semaphore_signal(barrier, inc=1, device_id=(s, other(h, stride)), device_id_type=MESH)

    mine_nope = pl.ds(pl.multiple_of(s * nope_cols, LANES), nope_cols)
    mine_rope = pl.ds(pl.multiple_of(s * rope_cols, LANES), rope_cols)
    mine_kv = pl.ds(pl.multiple_of(s * kv_width, LANES), kv_width)
    loads = [
        pltpu.make_async_copy(w_nope.at[:, mine_nope], own_q.at[:, pl.ds(0, nope_cols)], local.at[0]),
        pltpu.make_async_copy(w_rope.at[:, mine_rope], own_q.at[:, pl.ds(nope_cols, rope_cols)], local.at[1]),
        pltpu.make_async_copy(w_kv.at[:, mine_kv], own_kv, local.at[2]),
    ]
    for copy in loads:
        copy.start()

    def window(whole, lat, ps, ph):
        width = lat.shape[1]
        return whole.at[pl.ds(pl.multiple_of(ps * rows, rows), rows), pl.ds(pl.multiple_of(ph * width, LANES), width)]

    def rope_at(ps, ph):
        return rope_all.at[ps, pl.ds(pl.multiple_of(ph * part, part), part), :]

    def places(ps, ph):
        return window(q_all, q_lat, ps, ph), window(kv_all, kv_lat, ps, ph), rope_at(ps, ph)

    mine = (q_lat, kv_lat, rope.at[pl.ds(pl.multiple_of(h * part, part), part), :])
    send_sems = (q_send, kv_send, rope_send)
    recv_sems = (q_recv, kv_recv, rope_recv)
    stores = [
        pltpu.make_async_copy(src, dst, local.at[3 + i])
        for i, (src, dst) in enumerate(zip(mine + (segs,), places(s, h) + (segs_all.at[s],)))
    ]
    for copy in stores:
        copy.start()
    pl.semaphore_wait(barrier, n - 1 + len(strides))

    sends = []
    slots = [0]

    def piece(ps, ph, target, own):
        slot = slots[0]
        slots[0] += 1
        copies = [
            pltpu.make_async_remote_copy(
                src_ref=src, dst_ref=dst, send_sem=sent.at[slot], recv_sem=got.at[ps * m + ph],
                device_id=target, device_id_type=MESH)
            for src, dst, sent, got in zip(
                mine if own else places(ps, ph), places(ps, ph), send_sems, recv_sems)
        ]
        for copy in copies:
            copy.start()

        def drain():
            for sent, src in zip(send_sems, mine):
                pltpu.make_async_copy(src, src, sent.at[slot]).wait()

        sends.append(drain)

    def arrive(ps, ph):
        for at, got in zip(places(ps, ph), recv_sems):
            pltpu.make_async_copy(at, at, got.at[ps * m + ph]).wait()

    others = []

    def weights(k):
        p = lax.rem(s + k, n)
        to = (p, h)
        q_at = pl.ds(pl.multiple_of(s * q_rows, q_rows), q_rows)
        kv_at = pl.ds(pl.multiple_of(s * kv_rows, kv_rows), kv_rows)
        pairs = (
            (w_nope.at[:, pl.ds(pl.multiple_of(p * nope_cols, LANES), nope_cols)], q_cols.at[q_at, pl.ds(0, nope_cols)]),
            (w_rope.at[:, pl.ds(pl.multiple_of(p * rope_cols, LANES), rope_cols)], q_cols.at[q_at, pl.ds(nope_cols, rope_cols)]),
            (w_kv.at[:, pl.ds(pl.multiple_of(p * kv_width, LANES), kv_width)], kv_cols.at[kv_at, :]),
        )
        for i, (src, dst) in enumerate(pairs):
            copy = pltpu.make_async_remote_copy(
                src_ref=src, dst_ref=dst, send_sem=w_send.at[i * n + k], recv_sem=w_recv.at[i * n + k],
                device_id=to, device_id_type=MESH)
            copy.start()
            others.append(copy)

    pair = other(s, 1)
    even = list(range(2, n, 2))

    for k in even:
        piece(s, h, (lax.rem(s + k, n), h), True)
    piece(s, h, (pair, h), True)
    for stride in strides:
        piece(s, h, (s, other(h, stride)), True)
    for k in range(1, n):
        copy = pltpu.make_async_remote_copy(
            src_ref=segs, dst_ref=segs_all.at[s], send_sem=seg_send.at[k], recv_sem=seg_recv.at[k],
            device_id=(lax.rem(s + k, n), h), device_id_type=MESH)
        copy.start()
        others.append(copy)
    for k in even:
        weights(k)
    for k in even:
        ps = lax.rem(s + n - k, n)
        arrive(ps, h)
        piece(ps, h, (pair, h), False)
        for stride in strides:
            piece(ps, h, (s, other(h, stride)), False)
    for k in range(1, n, 2):
        weights(k)
    for copy in loads:
        copy.wait()
    keep = [
        pltpu.make_async_copy(own_q, q_cols.at[pl.ds(pl.multiple_of(s * q_rows, q_rows), q_rows), :], local.at[7]),
        pltpu.make_async_copy(own_kv, kv_cols.at[pl.ds(pl.multiple_of(s * kv_rows, kv_rows), kv_rows), :], local.at[8]),
    ]
    for copy in keep:
        copy.start()
    for k in [0] + even:
        ps = lax.rem(pair + n - k, n)
        arrive(ps, h)
        for stride in strides:
            piece(ps, h, (s, other(h, stride)), False)
    held = [h]
    for i, stride in enumerate(strides):
        fresh = [other(ph, stride) for ph in held]
        for first in range(n):
            ps = lax.rem(s + first, n)
            for ph in fresh:
                arrive(ps, ph)
                for later in strides[i + 1:]:
                    piece(ps, ph, (s, other(h, later)), False)
        held = held + fresh
    for copy in others:
        copy.wait()
    for drain in sends:
        drain()
    for copy in stores + keep:
        copy.wait()


def gather_all(n, m, q_lat, kv_lat, rope, segs, w_nope, w_rope, w_kv):
    rows = q_lat.shape[0]
    q_width = (w_nope.shape[1] + w_rope.shape[1]) // n
    kv_width = w_kv.shape[1] // n
    moves = n // 2 - 1 + n * m
    any_ref = pl.BlockSpec(memory_space=pl.ANY)
    vmem = pl.BlockSpec(memory_space=pltpu.VMEM)
    dma = pltpu.SemaphoreType.DMA
    return pl.pallas_call(
        functools.partial(gather_kernel, n, m),
        out_shape=(
            jax.ShapeDtypeStruct((n * rows, m * q_lat.shape[1]), q_lat.dtype),
            jax.ShapeDtypeStruct((n * rows, m * kv_lat.shape[1]), kv_lat.dtype),
            jax.ShapeDtypeStruct((n,) + rope.shape, rope.dtype),
            jax.ShapeDtypeStruct((n,) + segs.shape, segs.dtype),
            jax.ShapeDtypeStruct((n * w_nope.shape[0], q_width), w_nope.dtype),
            jax.ShapeDtypeStruct((n * w_kv.shape[0], kv_width), w_kv.dtype),
        ),
        in_specs=[vmem, vmem, vmem, vmem, any_ref, any_ref, any_ref],
        out_specs=(any_ref,) * 6,
        scratch_shapes=[
            pltpu.VMEM((w_nope.shape[0], q_width), w_nope.dtype),
            pltpu.VMEM((w_kv.shape[0], kv_width), w_kv.dtype),
            dma((moves,)), dma((n * m,)), dma((moves,)), dma((n * m,)), dma((moves,)), dma((n * m,)),
            dma((n,)), dma((n,)),
            dma((3 * n,)), dma((3 * n,)), dma((9,)),
        ],
        compiler_params=pltpu.CompilerParams(collective_id=0, has_side_effects=True),
        name="gather_all",
    )(q_lat, kv_lat, rope, segs, w_nope, w_rope, w_kv)


def logit_kernel(own, q_lat, kv_lat, rope, segs, w_q, w_kv, out, keys, seg_cols):
    block = pl.program_id(0)
    rows = q_lat.shape[0]
    window = (REACH + 1) * rows
    q_scale = 1.0 / math.sqrt(QLORA)
    k_scale = 1.0 / math.sqrt(KVLORA)
    key = (jnp.dot(kv_lat[...], w_kv[...], preferred_element_type=jnp.float32) * k_scale).astype(jnp.bfloat16)
    query = (jnp.dot(q_lat[...], w_q[...], preferred_element_type=jnp.float32) * q_scale).astype(jnp.bfloat16)
    here = pl.ds(pl.multiple_of(block * rows, rows), rows)
    lane = lax.broadcasted_iota(jnp.int32, (rows, LANES), 1)
    turned = jnp.concatenate([rope[0].astype(jnp.float32)] * (LANES // D_ROPE), 0)
    twice = jnp.transpose(turned).astype(jnp.bfloat16)
    sides = [
        jnp.where(lane // D_ROPE == side, twice, jnp.zeros_like(twice)) for side in range(LANES // D_ROPE)
    ]
    for i in range(own):
        keys[i, here, :] = jnp.concatenate(
            [key[:, i * D_NOPE : (i + 1) * D_NOPE], sides[i % len(sides)]], 1
        )
    seg_row = segs[0]
    seg_cols[here, :] = jnp.transpose(jnp.broadcast_to(seg_row, (LANES, rows)))
    start = jnp.maximum(block - REACH, 0) * rows
    range_keys = pl.ds(pl.multiple_of(start, rows), window)
    key_segs = seg_cols[range_keys, :]
    key_segs = jnp.concatenate([key_segs] * (rows // LANES), 1)
    key_pos = start + lax.broadcasted_iota(jnp.int32, (window, rows), 0)
    query_pos = block * rows + lax.broadcasted_iota(jnp.int32, (window, rows), 1)
    allowed = (key_segs == seg_row) & (key_pos <= query_pos)
    base = own * D_NOPE
    found = []
    for i in range(own):
        pair = base + i // len(sides) * LANES
        q_head = jnp.concatenate(
            [query[:, i * D_NOPE : (i + 1) * D_NOPE], query[:, pair : pair + LANES]], 1
        )
        logits = lax.dot_general(
            keys[i, range_keys, :], q_head, (((1,), (1,)), ((), ())), preferred_element_type=jnp.float32
        )
        logits = jnp.where(allowed, logits, jnp.float32(-1e30))
        found.append(jnp.max(logits, axis=0, keepdims=True))
    out[0:own, here] = jnp.concatenate(found, 0) * (1.0 / math.sqrt(D_NOPE + D_ROPE))

    @pl.when(block == pl.num_programs(0) - 1)
    def _():
        top = jnp.max(out[0:own, :], axis=1, keepdims=True)
        out[own : 2 * own, :] = jnp.broadcast_to(top, (own, out.shape[1]))


def logit_maxima(n, own, q_lat, kv_lat, rope, segs, w_q, w_kv):
    rows = q_lat.shape[0] // n
    return pl.pallas_call(
        functools.partial(logit_kernel, own),
        grid=(n,),
        out_shape=jax.ShapeDtypeStruct((2 * own, q_lat.shape[0]), jnp.float32),
        in_specs=[
            pl.BlockSpec((rows, q_lat.shape[1]), lambda i: (i, 0)),
            pl.BlockSpec((rows, kv_lat.shape[1]), lambda i: (i, 0)),
            pl.BlockSpec((1,) + rope.shape[1:], lambda i: (i, 0, 0)),
            pl.BlockSpec((1,) + segs.shape[1:], lambda i: (i, 0, 0)),
            pl.BlockSpec(w_q.shape, lambda i: (0, 0)),
            pl.BlockSpec(w_kv.shape, lambda i: (0, 0)),
        ],
        out_specs=pl.BlockSpec((2 * own, q_lat.shape[0]), lambda i: (0, 0)),
        scratch_shapes=[
            pltpu.VMEM((own, q_lat.shape[0], D_NOPE + LANES), jnp.bfloat16),
            pltpu.VMEM((q_lat.shape[0], LANES), jnp.int32),
        ],
        compiler_params=pltpu.CompilerParams(dimension_semantics=("arbitrary",)),
        name="logit_maxima",
    )(q_lat, kv_lat, rope, segs, w_q, w_kv)


def exchange_kernel(n, maxima, out, send, recv):
    s = lax.axis_index("seq")
    h = lax.axis_index("head")
    rows = out.shape[2]
    barrier = pltpu.get_barrier_semaphore()
    for k in range(1, n):
        pl.semaphore_signal(barrier, inc=1, device_id=(lax.rem(s + k, n), h), device_id_type=MESH)
    pl.semaphore_wait(barrier, n - 1)
    copies = []
    for k in range(1, n):
        p = lax.rem(s + k, n)
        copy = pltpu.make_async_remote_copy(
            src_ref=maxima.at[:, pl.ds(pl.multiple_of(p * rows, rows), rows)], dst_ref=out.at[s],
            send_sem=send.at[k], recv_sem=recv.at[k], device_id=(p, h), device_id_type=MESH)
        copy.start()
        copies.append(copy)
    out[s] = maxima[:, pl.ds(pl.multiple_of(s * rows, rows), rows)]
    for copy in copies:
        copy.wait()


def exchange(n, maxima):
    vmem = pl.BlockSpec(memory_space=pltpu.VMEM)
    return pl.pallas_call(
        functools.partial(exchange_kernel, n),
        out_shape=jax.ShapeDtypeStruct((n, maxima.shape[0], maxima.shape[1] // n), jnp.float32),
        in_specs=[vmem],
        out_specs=vmem,
        scratch_shapes=[pltpu.SemaphoreType.DMA((n,)), pltpu.SemaphoreType.DMA((n,))],
        compiler_params=pltpu.CompilerParams(collective_id=1, has_side_effects=True),
        name="exchange",
    )(maxima)


def owned_body(n, m, q_latent, kv_latent, k_rope, segment_ids, w_q_nope, w_q_rope, w_kv_nope, threshold):
    rows = q_latent.shape[0]
    heads = w_q_nope.shape[1] // D_NOPE
    own = heads // n
    gathered = gather_all(
        n, m, q_latent, kv_latent, k_rope.T, segment_ids.reshape(1, rows), w_q_nope, w_q_rope, w_kv_nope
    )
    maxima = logit_maxima(n, own, *gathered)
    got = exchange(n, maxima)
    row_max = got[:, :own, :].reshape(heads, rows).T
    head_max = got[:, own:, 0].reshape(heads)
    return finish(threshold, head_max, row_max, w_q_nope, w_q_rope, w_kv_nope)


def body(n, m, *operands):
    heads = operands[4].shape[1] // D_NOPE
    rows = operands[0].shape[0]
    shares = heads % n == 0 and heads // n % (LANES // D_ROPE) == 0
    fits = n % 2 == 0 and n > REACH and m & (m - 1) == 0 and rows % LANES == 0 and operands[2].shape[1] % (16 * m) == 0
    if shares and fits and heads // n % 4 == 0:
        return owned_body(n, m, *operands)
    return grouped_body(*operands)


def solution(mesh):
    in_specs = (
        P("seq", "head"),
        P("seq", "head"),
        P("seq", None),
        P("seq"),
        P("seq", "head"),
        P("seq", "head"),
        P("seq", "head"),
        P(),
    )
    out_specs = (P("seq", "head"), P("seq", "head"), P("seq", "head"), P("head"), P("seq", "head"))
    return jax.shard_map(functools.partial(body, mesh.shape["seq"], mesh.shape["head"]), mesh=mesh, in_specs=in_specs, out_specs=out_specs, check_vma=False)
```
